256 devices in a mesh: seq: 32 (over y, z), tp: 8 (over x, core).
Axes of the slice: x: 4, y: 4, z: 8, core: 2. Of those that a mesh axis runs over, the one named last changes fastest.
Arguments:
- tokens: bfloat16 [24576, 2048], P('seq', 'tp'), may hold values from -20 to 20
- w_query: bfloat16 [2048, 2048], P(None, 'tp'), may hold values from -0.125 to 0.125
- w_key: bfloat16 [2048, 2048], P(None, 'tp'), may hold values from -0.125 to 0.125
- w_value: bfloat16 [2048, 2048], P(None, 'tp'), may hold values from -0.125 to 0.125
- head_gain: float32 [2048], P('tp'), may hold values from 0.5 to 1.5
- w_out: bfloat16 [2048, 2048], P('tp'), may hold values from -0.125 to 0.125
- norm_gain: float32 [2048], replicated, may hold values from 0.5 to 1.5
- w_gate: bfloat16 [2048, 8192], P('seq', 'tp'), may hold values from -0.125 to 0.125
- w_up: bfloat16 [2048, 8192], P('seq', 'tp'), may hold values from -0.125 to 0.125
- w_down: bfloat16 [8192, 2048], P('tp', 'seq'), may hold values from -0.0625 to 0.0625
Outputs:
- layer_out: bfloat16 [24576, 2048], P('seq', 'tp')
The draws below stay inside these ranges and needn't reach their ends.
All inputs are finite; a program needn't handle non-finite values.
Results may differ from the reference program's by a relative error of at most 0.009.
Values may be sent and summed in bfloat16 or wider, within the bound.
No kernel may reach another device: no remote copies, remote signals or barrier semaphores. Data moves between devices by JAX's collectives and lax.ppermute only.
A program may use at most 128 MiB of HBM per device.

```python
import math
import jax
import jax.numpy as jnp
from jax import lax

D = 2048
HEADS = 16
HD = 128
FF = 8192
L_DEV = 768
TOKENS = 24576
N_SEQ = 32
N_TP = 8


def draw_tokens(key, part):
    key_base = jax.random.fold_in(key, 11)
    key_rows = jax.random.fold_in(key, 12)
    key_columns = jax.random.fold_in(key, 14)
    row_scale = jnp.exp(jax.random.uniform(key_rows, (TOKENS, 1), jnp.float32, math.log(0.5), math.log(5.0)))
    ramp = jnp.arange(D, dtype=jnp.float32)[None, :] / (D - 1.0)
    base = jax.random.normal(key_base, (TOKENS, D), jnp.float32)
    jitter = jax.random.uniform(key_columns, (1, D), jnp.float32, -0.15, 0.15)
    column_scale = jnp.exp(math.log(0.5) + ramp * math.log(4.0) + jitter)
    return jnp.clip(base * column_scale * row_scale, -20.0, 20.0).astype(jnp.bfloat16)


def shard_levels(key, extent, pieces, low, high):
    def one(position, blocks):
        steps = jax.random.uniform(jax.random.fold_in(jax.random.fold_in(key, 6), position), (blocks,), jnp.float32, low / len(pieces), high / len(pieces))
        return jnp.repeat(jnp.exp(steps), extent[position] // blocks).reshape((-1,) + (1,) * (len(extent) - position - 1))

    level = one(*pieces[0])
    for cut in pieces[1:]:
        level = level * one(*cut)
    return level


def centred(own_key, dims, scale, reach, split=(), kind=jnp.bfloat16):
    values = jax.random.normal(own_key, dims, jnp.float32) * scale
    if len(split) > 0:
        values = shard_levels(own_key, dims, split, -0.22, 0.18) * values
    return jnp.clip(values, min=-reach, max=reach).astype(kind)


def setup_inputs(seed: int = 0) -> dict:
    key_of = jax.random.split(jax.random.key(seed), 11)
    return {
        "tokens": draw_tokens(jax.random.fold_in(key_of[10], 71), 0),
        "w_query": centred(key_of[1], (D, D), D ** -0.5, 0.125, ((1, 8),)),
        "w_key": centred(key_of[2], (D, D), D ** -0.5, 0.125, ((1, 8),)),
        "w_value": centred(key_of[3], (D, D), D ** -0.5, 0.125, ((1, 8),)),
        "head_gain": jnp.clip(0.5 + 1.0 * jax.random.uniform(key_of[4], (D,), jnp.float32) ** shard_levels(key_of[4], (D,), ((0, 8),), -0.2, 0.2), 0.5, 1.5),
        "w_out": centred(key_of[5], (D, D), D ** -0.5, 0.125, ((0, 8),)),
        "norm_gain": jnp.clip(jax.random.uniform(key_of[6], (D,), jnp.float32, 0.5, 1.5), 0.5, 1.5),
        "w_gate": centred(key_of[7], (D, FF), D ** -0.5, 0.125, ((0, 32), (1, 8))),
        "w_up": centred(key_of[8], (D, FF), D ** -0.5, 0.125, ((0, 32), (1, 8))),
        "w_down": centred(key_of[9], (FF, D), FF ** -0.5, 0.0625, ((0, 8), (1, 32))),
    }


def reference(tokens, w_query, w_key, w_value, head_gain, w_out, norm_gain, w_gate, w_up, w_down):

    def project(weight):
        return jnp.dot(tokens, weight, preferred_element_type=jnp.float32).astype(jnp.bfloat16)
    query = project(w_query).reshape(N_SEQ, L_DEV, HEADS, HD)
    keys_all = project(w_key).reshape(N_SEQ, L_DEV, HEADS, HD)
    values_all = project(w_value).reshape(N_SEQ, L_DEV, HEADS, HD)
    causal = jnp.arange(L_DEV)[:, None] >= jnp.arange(L_DEV)[None, :]

    def block_step(state, inputs):
        query_block, key_block, value_block = inputs
        qf = query_block.astype(jnp.float32)
        kf = key_block.astype(jnp.float32)
        vf = value_block.astype(jnp.float32)
        scores = jnp.einsum('ihd,jhd->hij', qf, kf)
        scores = jnp.where(causal[None], scores, 0.0).astype(jnp.bfloat16)
        inside = jnp.einsum('hij,jhd->ihd', scores.astype(jnp.float32), vf)
        history = state.astype(jnp.bfloat16).astype(jnp.float32)
        carried = jnp.einsum('ihd,hde->ihe', qf, history)
        new_state = state + jnp.einsum('jhd,jhe->hde', kf, vf)
        return (new_state, inside + carried)
    start_state = jnp.zeros((HEADS, HD, HD), jnp.float32)
    final_state, mixed = lax.scan(block_step, start_state, (query, keys_all, values_all))
    mixed = mixed.reshape(TOKENS, HEADS, HD)
    scale = lax.rsqrt(lax.optimization_barrier(jnp.mean(mixed * mixed, axis=-1, keepdims=True)) + 1e-06)
    normed = (mixed * scale * head_gain.reshape(HEADS, HD)).astype(jnp.bfloat16).reshape(TOKENS, D)
    group_width = D // N_TP
    resid = tokens.astype(jnp.float32)
    for group in range(N_TP):
        lo = group * group_width
        part = jnp.dot(normed[:, lo:lo + group_width], w_out[lo:lo + group_width, :], preferred_element_type=jnp.float32)
        resid = resid + part.astype(jnp.bfloat16).astype(jnp.float32)
    factor = lax.rsqrt(lax.optimization_barrier(jnp.mean(resid * resid, axis=-1, keepdims=True)) + 1e-05)
    ffn_in = (resid * factor * norm_gain).astype(jnp.bfloat16)
    gate = jnp.dot(ffn_in, w_gate, preferred_element_type=jnp.float32)
    upward = jnp.dot(ffn_in, w_up, preferred_element_type=jnp.float32)
    hidden = (jax.nn.silu(gate) * upward).astype(jnp.bfloat16)
    hidden_width = FF // N_TP
    result = resid
    for group in range(N_TP):
        lo = group * hidden_width
        part = jnp.dot(hidden[:, lo:lo + hidden_width], w_down[lo:lo + hidden_width, :], preferred_element_type=jnp.float32)
        result = result + part.astype(jnp.bfloat16).astype(jnp.float32)
    return result.astype(jnp.bfloat16)
```

```python
import jax
import jax.numpy as jnp
from jax import lax
from jax.experimental import pallas as pl
from jax.experimental.pallas import tpu as pltpu
from jax.sharding import Mesh
from jax.sharding import PartitionSpec as P

HD = 128
W = 256
SEQ = ("y", "z")
TP = ("x", "core")
BF = jnp.bfloat16
F32 = jnp.float32


def shift(a, axis, by):
    n = lax.axis_size(axis)
    return lax.ppermute(a, axis, [(i, (i + by) % n) for i in range(n)])


def swap(a):
    return shift(a, "core", 1)


def spread(t):
    mine = [t, *(shift(t, "x", d) for d in (1, 2, 3))]
    return mine, [swap(m) for m in mine]


def params(n, flops=0):
    return dict(
        compiler_params=pltpu.CompilerParams(dimension_semantics=("arbitrary",) * n),
        cost_estimate=pl.CostEstimate(flops=flops, bytes_accessed=8 << 20, transcendentals=0),
    )


def dot(a, b, dims=((1,), (0,))):
    return lax.dot_general(a, b, (dims, ((), ())), preferred_element_type=F32)


def lay_out(place, mine, theirs, whole):
    x, core = place[0], place[1]
    for d in range(4):
        chip = lax.rem(x + 4 - d, 4)
        at = pl.multiple_of((2 * chip + core) * W, W)
        whole[:, pl.ds(at, W)] = mine[d][...]
        at = pl.multiple_of((2 * chip + 1 - core) * W, W)
        whole[:, pl.ds(at, W)] = theirs[d][...]


def keys_kernel(place, *refs):
    mine, theirs = refs[:4], refs[4:8]
    w_key, w_value, whole, keys, values, state, total = refs[8:]
    step = pl.program_id(0)
    lay_out(place, mine, theirs, whole)
    x = whole[...]
    k = dot(x, w_key[...]).astype(BF)
    v = dot(x, w_value[...]).astype(BF)
    keys[...] = k
    values[...] = v

    @pl.when(step == 0)
    def _():
        total[...] = jnp.zeros_like(total)

    for h in range(2):
        cols = slice(h * HD, (h + 1) * HD)
        total[h] += dot(k[:, cols], v[:, cols], ((0,), (0,)))

    @pl.when(step == pl.num_programs(0) - 1)
    def _():
        state[...] = total[...].astype(BF)


def inside_kernel(whole, w_query, keys, values, query, inside):
    rows, length = whole.shape[0], keys.shape[0]
    q = dot(whole[...], w_query[...]).astype(BF)
    query[...] = q
    i = lax.broadcasted_iota(jnp.int32, (rows, length), 0) + pl.program_id(0) * rows
    j = lax.broadcasted_iota(jnp.int32, (rows, length), 1)
    for h in range(2):
        cols = slice(h * HD, (h + 1) * HD)
        s = dot(q[:, cols], keys[:, cols], ((1,), (1,)))
        s = jnp.where(i >= j, s, 0.0).astype(BF)
        inside[:, cols] = dot(s, values[:, cols])


def mixed_kernel(place, query, inside, history, head_gain, w_keep, w_give, keep, give, normed):
    @pl.when(pl.program_id(0) == 0)
    def _():
        for h in range(2):
            cols = slice(h * HD, (h + 1) * HD)
            m = inside[:, cols] + dot(query[:, cols], history[h])
            scale = lax.rsqrt(jnp.mean(m * m, axis=-1, keepdims=True) + 1e-06)
            normed[:, cols] = (m * scale * head_gain[:, cols]).astype(BF)

    keep[0] = dot(normed[...], w_keep[...]).astype(BF)
    give[0] = dot(normed[...], w_give[...]).astype(BF)


def ffn_kernel(place, *refs):
    mine, theirs = refs[:4], refs[4:8]
    norm_gain, w_gate, w_up, w_keep, w_give, keep, give, ffn_in, hidden = refs[8:]
    step = pl.program_id(0)

    @pl.when(step == 0)
    def _():
        lay_out(place, mine, theirs, ffn_in)
        rows = 128

        def normalise(r, _):
            at = pl.ds(pl.multiple_of(r * rows, rows), rows)
            v = ffn_in[at, :].astype(F32)
            factor = lax.rsqrt(jnp.mean(v * v, axis=-1, keepdims=True) + 1e-05)
            ffn_in[at, :] = (v * factor * norm_gain[...]).astype(BF)
            return 0

        lax.fori_loop(0, ffn_in.shape[0] // rows, normalise, 0)

    for s in range(4):

        @pl.when(step == s)
        def _():
            g = dot(ffn_in[...], w_gate[...])
            u = dot(ffn_in[...], w_up[...])
            hidden[:, s * W : (s + 1) * W] = (g / (1.0 + jnp.exp(-g)) * u).astype(BF)

    @pl.when(step >= 4)
    def _():
        keep[0] = dot(hidden[...], w_keep[...], ((1,), (1,))).astype(BF)
        give[0] = dot(hidden[...], w_give[...], ((1,), (1,))).astype(BF)


def sum_at_owner(keep, give):
    x = lax.axis_index("x")
    both = keep.astype(F32) + swap(give).astype(F32)
    both = both.astype(BF)
    total = lax.dynamic_index_in_dim(both, x, 0, False).astype(F32)
    for d in (2, 1, 3):
        piece = lax.dynamic_index_in_dim(both, lax.rem(x + d, 4), 0, False)
        total = total + shift(piece, "x", d).astype(F32)
    return total


def earlier_blocks(state):
    z, y = lax.axis_index("z"), lax.axis_index("y")
    whole_row = state.astype(F32)
    before = jnp.zeros_like(whole_row)
    for d in (4, 3, 5, 2, 6, 1, 7):
        s = shift(state, "z", d).astype(F32)
        whole_row = whole_row + s
        before = before + jnp.where(z >= d, s, 0.0)
    row = whole_row.astype(BF)
    for d in (2, 1, 3):
        before = before + jnp.where(y >= d, shift(row, "y", d).astype(F32), 0.0)
    return before.astype(BF)


def body(tokens, w_query, w_key, w_value, head_gain, w_out, norm_gain, w_gate, w_up, w_down):
    length = tokens.shape[0]
    width = norm_gain.shape[0]
    heads = w_query.shape[1] // HD
    hidden = w_gate.shape[1]
    place = jnp.stack([lax.axis_index("x"), lax.axis_index("core")]).astype(jnp.int32)
    packed = jnp.concatenate([w_gate, w_up, w_down.T], axis=1)
    weights = lax.all_gather(packed, SEQ, axis=0, tiled=True)
    mine, theirs = spread(tokens)

    tile = 256
    piece = pl.BlockSpec((tile, W), lambda i, *_: (i, 0))
    row = pl.BlockSpec((tile, width), lambda i, *_: (i, 0))

    def full(*shape):
        return pl.BlockSpec(shape, lambda *_: (0,) * len(shape))

    whole, keys, values, state = pl.pallas_call(
        keys_kernel,
        grid_spec=pltpu.PrefetchScalarGridSpec(
            num_scalar_prefetch=1,
            grid=(length // tile,),
            in_specs=[piece] * 8 + [full(width, W)] * 2,
            out_specs=[row, piece, piece, full(heads, HD, HD)],
            scratch_shapes=[pltpu.VMEM((heads, HD, HD), F32)],
        ),
        out_shape=[
            jax.ShapeDtypeStruct((length, width), BF),
            jax.ShapeDtypeStruct((length, W), BF),
            jax.ShapeDtypeStruct((length, W), BF),
            jax.ShapeDtypeStruct((heads, HD, HD), BF),
        ],
        name="keys",
        **params(1, 4 * length * width * W),
    )(place, *mine, *theirs, w_key, w_value)
    history = earlier_blocks(state)
    query, inside = pl.pallas_call(
        inside_kernel,
        grid=(length // tile,),
        in_specs=[row, full(width, W), full(length, W), full(length, W)],
        out_specs=[piece, piece],
        out_shape=[
            jax.ShapeDtypeStruct((length, W), BF),
            jax.ShapeDtypeStruct((length, W), F32),
        ],
        name="inside",
        **params(1, 4 * length * width * W),
    )(whole, w_query, keys, values)

    out = jax.ShapeDtypeStruct((4, length, W), BF)
    keep, give = pl.pallas_call(
        mixed_kernel,
        grid_spec=pltpu.PrefetchScalarGridSpec(
            num_scalar_prefetch=1,
            grid=(4,),
            in_specs=[
                full(length, W),
                full(length, W),
                full(heads, HD, HD),
                full(1, W),
                pl.BlockSpec((W, W), lambda i, p: (0, 2 * i + p[1])),
                pl.BlockSpec((W, W), lambda i, p: (0, 2 * i + 1 - p[1])),
            ],
            out_specs=[pl.BlockSpec((1, length, W), lambda i, p: (i, 0, 0))] * 2,
            scratch_shapes=[pltpu.VMEM((length, W), BF)],
        ),
        out_shape=[out, out],
        name="mixed",
        **params(1, 2 * length * width * W),
    )(place, query, inside, history, head_gain.reshape(1, W), w_out, w_out)
    resid = tokens.astype(F32) + sum_at_owner(keep, give)
    mine, theirs = spread(resid.astype(BF))

    def first(i):
        return jnp.minimum(i, 3)

    def second(i):
        return jnp.maximum(i - 4, 0)

    n = hidden // W
    keep, give = pl.pallas_call(
        ffn_kernel,
        grid_spec=pltpu.PrefetchScalarGridSpec(
            num_scalar_prefetch=1,
            grid=(8,),
            in_specs=[full(length, W)] * 8
            + [
                full(1, width),
                pl.BlockSpec((width, W), lambda i, p: (0, first(i))),
                pl.BlockSpec((width, W), lambda i, p: (0, n + first(i))),
                pl.BlockSpec((W, hidden), lambda i, p: (2 * second(i) + p[1], 2)),
                pl.BlockSpec((W, hidden), lambda i, p: (2 * second(i) + 1 - p[1], 2)),
            ],
            out_specs=[pl.BlockSpec((1, length, W), lambda i, p: (second(i), 0, 0))] * 2,
            scratch_shapes=[pltpu.VMEM((length, width), BF), pltpu.VMEM((length, hidden), BF)],
        ),
        out_shape=[out, out],
        name="ffn",
        **params(1, 6 * length * width * hidden),
    )(place, *mine, *theirs, norm_gain.reshape(1, width), weights, weights, weights, weights)
    return (resid + sum_at_owner(keep, give)).astype(BF)


def solution(mesh):
    finer = Mesh(mesh.devices.reshape(4, 8, 4, 2), SEQ + TP)
    return jax.shard_map(
        body,
        mesh=finer,
        in_specs=(
            P(SEQ, TP),
            P(None, TP),
            P(None, TP),
            P(None, TP),
            P(TP),
            P(TP, None),
            P(),
            P(SEQ, TP),
            P(SEQ, TP),
            P(TP, SEQ),
        ),
        out_specs=P(SEQ, TP),
        check_vma=False,
    )
```

```python
import functools

import jax
import jax.numpy as jnp
from jax import lax
from jax.experimental import pallas as pl
from jax.experimental.pallas import tpu as pltpu
from jax.sharding import Mesh
from jax.sharding import PartitionSpec as P


HD = 128
W = 256
SEQ = ("y", "z")
TP = ("x", "core")
BF = jnp.bfloat16
F32 = jnp.float32


def shift(a, axis, by):
    n = lax.axis_size(axis)
    return lax.ppermute(a, axis, [(i, (i + by) % n) for i in range(n)])


def swap(a):
    return shift(a, "core", 1)


def spread(t):
    mine, theirs = [t], []
    for d in (1, 2, 3):
        mine.append(shift(t, "x", d))
    for d in range(4):
        theirs.append(swap(mine[d]))
    return mine, theirs


def here(a):
    return pltpu.with_memory_space_constraint(a, pltpu.VMEM)


def kernel_of(body, out, *args, scratch=(), flops=0, grant=8):
    place = pl.BlockSpec(memory_space=pltpu.SMEM)
    vmem = pl.BlockSpec(memory_space=pltpu.VMEM)
    stays = pl.BlockSpec(memory_space=pltpu.HBM)
    specs, values = [], []
    for a in args:
        if isinstance(a, tuple):
            specs.append(stays)
            values.append(pltpu.with_memory_space_constraint(a[0], pltpu.HBM))
        elif a.dtype == jnp.int32:
            specs.append(place)
            values.append(a)
        else:
            specs.append(vmem)
            values.append(here(a))
    return pl.pallas_call(
        body,
        in_specs=specs,
        out_specs=[stays if space else vmem for _, _, *space in out],
        out_shape=[(space or [pltpu.VMEM])[0](shape, dtype) for shape, dtype, *space in out],
        scratch_shapes=list(scratch),
        compiler_params=pltpu.CompilerParams(vmem_limit_bytes=grant << 20),
        cost_estimate=pl.CostEstimate(flops=flops, bytes_accessed=8 << 20, transcendentals=0),
    )(*values)


def dot(a, b, dims=((1,), (0,))):
    return lax.dot_general(a, b, (dims, ((), ())), preferred_element_type=F32)


def pieces_of(place, mine, theirs):
    x, core = place[0], place[1]
    for d in range(4):
        chip = lax.rem(x + 4 - d, 4)
        yield pl.multiple_of((2 * chip + core) * W, W), mine[d]
        yield pl.multiple_of((2 * chip + 1 - core) * W, W), theirs[d]


def by_tiles(length, step):
    def run(i, _):
        step(pl.ds(pl.multiple_of(i * 256, 256), 256))
        return 0

    lax.fori_loop(0, length // 256, run, 0)


def keys_kernel(place, *refs):
    k_from, v_from, whole, keys, values, state, w_key, w_value, sems = refs[8:]
    load_k = pltpu.make_async_copy(k_from, w_key, sems.at[0])
    load_v = pltpu.make_async_copy(v_from, w_value, sems.at[1])
    load_k.start()
    load_v.start()

    @functools.partial(by_tiles, whole.shape[0])
    def _(rows):
        for at, piece in pieces_of(place, refs[:4], refs[4:8]):
            whole[rows, pl.ds(at, W)] = piece[rows, :]

    load_k.wait()
    load_v.wait()

    @functools.partial(by_tiles, whole.shape[0])
    def _(rows):
        keys[rows, :] = dot(whole[rows, :], w_key[...]).astype(BF)
        values[rows, :] = dot(whole[rows, :], w_value[...]).astype(BF)

    for h in range(2):
        cols = slice(h * HD, (h + 1) * HD)
        state[h] = dot(keys[:, cols], values[:, cols], ((0,), (0,))).astype(BF)


def query_kernel(whole, w_query, query):
    @functools.partial(by_tiles, whole.shape[0])
    def _(rows):
        query[rows, :] = dot(whole[rows, :], w_query[...]).astype(BF)


def inside_kernel(query, keys, values, inside):
    length = keys.shape[0]

    @functools.partial(by_tiles, length)
    def _(rows):
        i = lax.broadcasted_iota(jnp.int32, (256, length), 0) + rows.start
        j = lax.broadcasted_iota(jnp.int32, (256, length), 1)
        for h in range(2):
            cols = slice(h * HD, (h + 1) * HD)
            s = dot(query[rows, cols], keys[:, cols], ((1,), (1,)))
            s = jnp.where(i >= j, s, 0.0).astype(BF)
            inside[rows, cols] = dot(s, values[:, cols])


def mixed_kernel(query, inside, history, head_gain, normed):
    @functools.partial(by_tiles, query.shape[0])
    def _(rows):
        for h in range(2):
            cols = slice(h * HD, (h + 1) * HD)
            m = inside[rows, cols] + dot(query[rows, cols], history[h])
            scale = lax.rsqrt(jnp.mean(m * m, axis=-1, keepdims=True) + 1e-06)
            normed[rows, cols] = (m * scale * head_gain[:, cols]).astype(BF)


def prep_kernel(place, *refs):
    norm_gain, scaled_out, factor_out, scaled, factor, sems = refs[8:]
    length, width = scaled.shape

    @functools.partial(by_tiles, length)
    def _(rows):
        total = jnp.zeros((256, W), F32)
        for at, piece in pieces_of(place, refs[:4], refs[4:8]):
            v = piece[rows, :].astype(F32)
            total = total + v * v
            scaled[rows, pl.ds(at, W)] = (v * norm_gain[:, pl.ds(at, W)]).astype(BF)
        mean = jnp.sum(total, axis=-1, keepdims=True) / width
        factor[rows, :] = jnp.broadcast_to(lax.rsqrt(mean + 1e-05), (256, factor.shape[1]))

    copies = [
        pltpu.make_async_copy(scaled, scaled_out, sems.at[0]),
        pltpu.make_async_copy(factor, factor_out, sems.at[1]),
    ]
    for c in copies:
        c.start()
    for c in copies:
        c.wait()


def hidden_kernel(scaled_from, factor_from, weights, hidden, downs, x, factor, gate, up, sems):
    length, _ = x.shape
    ff = hidden.shape[1]

    def tile(s):
        at = pl.multiple_of(s * W, W)
        g = pltpu.make_async_copy(weights.at[:, pl.ds(at, W)], gate.at[s], sems.at[0, s])
        u = pltpu.make_async_copy(weights.at[:, pl.ds(ff + at, W)], up.at[s], sems.at[1, s])
        return g, u

    def rows_of(r):
        rows = pl.ds(r * W, W)
        return pltpu.make_async_copy(scaled_from.at[rows, :], x.at[rows, :], sems.at[2, r])

    scales = pltpu.make_async_copy(factor_from, factor, sems.at[2, 3])
    last = pltpu.make_async_copy(weights.at[:, 2 * ff : 3 * ff], downs, sems.at[3, 0])
    rows_of(0).start()
    for c in tile(0):
        c.start()
    scales.start()
    for r in range(1, length // W):
        rows_of(r).start()
    for s in range(1, ff // W):
        for c in tile(s):
            c.start()
    last.start()

    def step(s, _):
        for c in tile(s):
            c.wait()
        cols = pl.ds(pl.multiple_of(s * W, W), W)

        @pl.when(s == 0)
        def _():
            scales.wait()

        for r in range(length // W):

            @pl.when(s == 0)
            def _():
                rows_of(r).wait()

            rows = slice(r * W, (r + 1) * W)
            f = jnp.concatenate([factor[rows, :]] * (W // factor.shape[1]), axis=1)
            g = dot(x[rows, :], gate[s]) * f
            u = dot(x[rows, :], up[s]) * f
            hidden[rows, cols] = (g / (1.0 + jnp.exp(-g)) * u).astype(BF)
        return 0

    lax.fori_loop(0, ff // W, step, 0)
    last.wait()


def sum_at_owner(part, base):
    arrived = {}
    for d in (2, 1, 3, 0):
        core = lax.axis_index("core")
        give = part(d, 1 - core)
        got = swap(give)
        keep = part(d, core)
        both = keep.astype(F32) + got.astype(F32)
        if d == 0:
            both = base + both
        else:
            both = shift(both.astype(BF), "x", d).astype(F32)
        arrived[d] = both
    return arrived[0] + arrived[1] + arrived[2] + arrived[3]


def earlier_blocks(state, fillers):
    z, y = lax.axis_index("z"), lax.axis_index("y")
    other = lax.ppermute(state, "z", [(i, i ^ 1) for i in range(lax.axis_size("z"))]).astype(F32)
    row = state.astype(F32) + other
    before = jnp.where(z % 2 == 1, other, 0.0)
    pair = row.astype(BF)
    found = [shift(pair, "z", d) for d in (4, 2, 6)]
    filled = fillers()
    *found, filled = lax.optimization_barrier((*found, filled))
    for d, s in zip((4, 2, 6), found):
        s = s.astype(F32)
        row = row + s
        before = before + jnp.where(z >= d, s, 0.0)
    row = row.astype(BF)
    for d in (2, 1, 3):
        before = before + jnp.where(y >= d, shift(row, "y", d).astype(F32), 0.0)
    return before.astype(BF), filled


def body(tokens, w_query, w_key, w_value, head_gain, w_out, norm_gain, w_gate, w_up, w_down):
    length = tokens.shape[0]
    width = norm_gain.shape[0]
    heads = w_query.shape[1] // HD
    ff = w_gate.shape[1]
    place = jnp.stack([lax.axis_index(a) for a in ("x", "core")]).astype(jnp.int32)
    packed = jnp.concatenate([w_gate, w_up, w_down.T], axis=1)
    weights = lax.all_gather(packed, SEQ, axis=0, tiled=True)
    mine, theirs = spread(tokens)
    rows, row = (length, W), (length, width)
    whole, keys, values, state = kernel_of(
        keys_kernel,
        [(row, BF), (rows, BF), (rows, BF), ((heads, HD, HD), BF)],
        place,
        *mine,
        *theirs,
        (w_key,),
        (w_value,),
        scratch=[
            pltpu.VMEM((width, W), BF),
            pltpu.VMEM((width, W), BF),
            pltpu.SemaphoreType.DMA((2,)),
        ],
        flops=4 * length * width * W,
    )

    def query_of():
        return kernel_of(
            query_kernel, [(rows, BF)], whole, w_query, flops=2 * length * width * W
        )[0]

    history, query = earlier_blocks(state, query_of)
    (inside,) = kernel_of(
        inside_kernel, [(rows, F32)], query, keys, values, flops=4 * length * length * W
    )
    (normed,) = kernel_of(
        mixed_kernel,
        [(rows, BF)],
        query,
        inside,
        history,
        head_gain.reshape(1, W),
        flops=2 * length * HD * W,
    )
    x = lax.axis_index("x")

    def attn(d, c):
        at = (2 * lax.rem(x + d, 4) + c) * W
        return dot(normed, lax.dynamic_slice_in_dim(w_out, at, W, 1)).astype(BF)

    resid = sum_at_owner(attn, tokens)
    mine, theirs = spread(resid.astype(BF))
    n = ff // W
    scaled, factor = kernel_of(
        prep_kernel,
        [(row, BF, pltpu.HBM), ((length, HD), F32, pltpu.HBM)],
        place,
        *mine,
        *theirs,
        norm_gain.reshape(1, width),
        scratch=[
            pltpu.VMEM(row, BF),
            pltpu.VMEM((length, HD), F32),
            pltpu.SemaphoreType.DMA((2,)),
        ],
        flops=4 * length * width,
    )
    hidden, downs = kernel_of(
        hidden_kernel,
        [((length, ff), BF), ((width, ff), BF)],
        (scaled,),
        (factor,),
        (weights,),
        scratch=[
            pltpu.VMEM(row, BF),
            pltpu.VMEM((length, HD), F32),
            pltpu.VMEM((n, width, W), BF),
            pltpu.VMEM((n, width, W), BF),
            pltpu.SemaphoreType.DMA((4, 4)),
        ],
        flops=4 * length * width * ff,
        grant=20,
    )

    def mlp(d, c):
        at = (2 * lax.rem(x + d, 4) + c) * W
        w = lax.dynamic_slice_in_dim(downs, at, W, 0)
        return dot(hidden, w, ((1,), (1,))).astype(BF)

    return sum_at_owner(mlp, resid).astype(BF)


def solution(mesh):
    finer = Mesh(mesh.devices.reshape(4, 8, 4, 2), SEQ + TP)
    return jax.shard_map(
        body,
        mesh=finer,
        in_specs=(
            P(SEQ, TP),
            P(None, TP),
            P(None, TP),
            P(None, TP),
            P(TP),
            P(TP, None),
            P(),
            P(SEQ, TP),
            P(SEQ, TP),
            P(TP, SEQ),
        ),
        out_specs=P(SEQ, TP),
        check_vma=False,
    )
```

```python
import functools

import jax
import jax.numpy as jnp
from jax import lax
from jax.experimental import pallas as pl
from jax.experimental.pallas import tpu as pltpu
from jax.sharding import Mesh
from jax.sharding import PartitionSpec as P


HD = 128
W = 256
SEQ = ("y", "z")
TP = ("x", "core")
BF = jnp.bfloat16
F32 = jnp.float32


def shift(a, axis, by):
    n = lax.axis_size(axis)
    return lax.ppermute(a, axis, [(i, (i + by) % n) for i in range(n)])


def swap(a):
    return shift(a, "core", 1)


def spread(t):
    mine, theirs = [t], []
    for d in (1, 2, 3):
        mine.append(shift(t, "x", d))
    for d in range(4):
        theirs.append(swap(mine[d]))
    return mine, theirs


def here(a):
    return pltpu.with_memory_space_constraint(a, pltpu.VMEM)


def kernel_of(body, out, *args, scratch=(), flops=0, grant=8):
    place = pl.BlockSpec(memory_space=pltpu.SMEM)
    vmem = pl.BlockSpec(memory_space=pltpu.VMEM)
    stays = pl.BlockSpec(memory_space=pltpu.HBM)
    specs, values = [], []
    for a in args:
        if isinstance(a, tuple):
            specs.append(stays)
            values.append(pltpu.with_memory_space_constraint(a[0], pltpu.HBM))
        elif a.dtype == jnp.int32:
            specs.append(place)
            values.append(a)
        else:
            specs.append(vmem)
            values.append(here(a))
    return pl.pallas_call(
        body,
        in_specs=specs,
        out_specs=[stays if space else vmem for _, _, *space in out],
        out_shape=[(space or [pltpu.VMEM])[0](shape, dtype) for shape, dtype, *space in out],
        scratch_shapes=list(scratch),
        compiler_params=pltpu.CompilerParams(vmem_limit_bytes=grant << 20),
        cost_estimate=pl.CostEstimate(flops=flops, bytes_accessed=8 << 20, transcendentals=0),
    )(*values)


def dot(a, b, dims=((1,), (0,))):
    return lax.dot_general(a, b, (dims, ((), ())), preferred_element_type=F32)


def pieces_of(place, mine, theirs):
    x, core = place[0], place[1]
    for d in range(4):
        chip = lax.rem(x + 4 - d, 4)
        yield pl.multiple_of((2 * chip + core) * W, W), mine[d]
        yield pl.multiple_of((2 * chip + 1 - core) * W, W), theirs[d]


def by_tiles(length, step):
    def run(i, _):
        step(pl.ds(pl.multiple_of(i * 256, 256), 256))
        return 0

    lax.fori_loop(0, length // 256, run, 0)


def keys_kernel(place, *refs):
    k_from, v_from, whole, keys, values, state, w_key, w_value, sems = refs[8:]
    load_k = pltpu.make_async_copy(k_from, w_key, sems.at[0])
    load_v = pltpu.make_async_copy(v_from, w_value, sems.at[1])
    load_k.start()
    load_v.start()

    @functools.partial(by_tiles, whole.shape[0])
    def _(rows):
        for at, piece in pieces_of(place, refs[:4], refs[4:8]):
            whole[rows, pl.ds(at, W)] = piece[rows, :]

    load_k.wait()
    load_v.wait()

    @functools.partial(by_tiles, whole.shape[0])
    def _(rows):
        keys[rows, :] = dot(whole[rows, :], w_key[...]).astype(BF)
        values[rows, :] = dot(whole[rows, :], w_value[...]).astype(BF)

    for h in range(2):
        cols = slice(h * HD, (h + 1) * HD)
        state[h] = dot(keys[:, cols], values[:, cols], ((0,), (0,))).astype(BF)


def query_kernel(whole, w_query, query):
    @functools.partial(by_tiles, whole.shape[0])
    def _(rows):
        query[rows, :] = dot(whole[rows, :], w_query[...]).astype(BF)


def inside_kernel(query, keys, values, inside):
    length = keys.shape[0]

    @functools.partial(by_tiles, length)
    def _(rows):
        i = lax.broadcasted_iota(jnp.int32, (256, length), 0) + rows.start
        j = lax.broadcasted_iota(jnp.int32, (256, length), 1)
        for h in range(2):
            cols = slice(h * HD, (h + 1) * HD)
            s = dot(query[rows, cols], keys[:, cols], ((1,), (1,)))
            s = jnp.where(i >= j, s, 0.0).astype(BF)
            inside[rows, cols] = dot(s, values[:, cols])


def mixed_kernel(query, inside, history, head_gain, normed):
    @functools.partial(by_tiles, query.shape[0])
    def _(rows):
        for h in range(2):
            cols = slice(h * HD, (h + 1) * HD)
            m = inside[rows, cols] + dot(query[rows, cols], history[h])
            scale = lax.rsqrt(jnp.mean(m * m, axis=-1, keepdims=True) + 1e-06)
            normed[rows, cols] = (m * scale * head_gain[:, cols]).astype(BF)


def prep_kernel(place, *refs):
    norm_gain, scaled_out, factor_out, scaled, factor, sems = refs[8:]
    length, width = scaled.shape

    @functools.partial(by_tiles, length)
    def _(rows):
        total = jnp.zeros((256, W), F32)
        for at, piece in pieces_of(place, refs[:4], refs[4:8]):
            v = piece[rows, :].astype(F32)
            total = total + v * v
            scaled[rows, pl.ds(at, W)] = (v * norm_gain[:, pl.ds(at, W)]).astype(BF)
        mean = jnp.sum(total, axis=-1, keepdims=True) / width
        factor[rows, :] = jnp.broadcast_to(lax.rsqrt(mean + 1e-05), (256, factor.shape[1]))

    copies = [
        pltpu.make_async_copy(scaled, scaled_out, sems.at[0]),
        pltpu.make_async_copy(factor, factor_out, sems.at[1]),
    ]
    for c in copies:
        c.start()
    for c in copies:
        c.wait()


def hidden_kernel(scaled_from, factor_from, weights, hidden, downs, x, factor, gate, up, sems):
    length, _ = x.shape
    ff = hidden.shape[1]

    def tile(s):
        at = pl.multiple_of(s * W, W)
        g = pltpu.make_async_copy(weights.at[:, pl.ds(at, W)], gate.at[s], sems.at[0, s])
        u = pltpu.make_async_copy(weights.at[:, pl.ds(ff + at, W)], up.at[s], sems.at[1, s])
        return g, u

    def rows_of(r):
        rows = pl.ds(r * W, W)
        return pltpu.make_async_copy(scaled_from.at[rows, :], x.at[rows, :], sems.at[2, r])

    scales = pltpu.make_async_copy(factor_from, factor, sems.at[2, 3])
    last = pltpu.make_async_copy(weights.at[:, 2 * ff : 3 * ff], downs, sems.at[3, 0])
    rows_of(0).start()
    for c in tile(0):
        c.start()
    scales.start()
    for r in range(1, length // W):
        rows_of(r).start()
    for s in range(1, ff // W):
        for c in tile(s):
            c.start()
    last.start()

    scales.wait()
    for r in range(length // W):
        rows_of(r).wait()

    def step(s, _):
        for c in tile(s):
            c.wait()
        cols = pl.ds(pl.multiple_of(s * W, W), W)

        for r in range(length // W):
            rows = slice(r * W, (r + 1) * W)
            f = jnp.concatenate([factor[rows, :]] * (W // factor.shape[1]), axis=1)
            g = dot(x[rows, :], gate[s]) * f
            u = dot(x[rows, :], up[s]) * f
            hidden[rows, cols] = (g / (1.0 + jnp.exp(-g)) * u).astype(BF)
        return 0

    lax.fori_loop(0, ff // W, step, 0)
    last.wait()


def halves_of(part):
    core = lax.axis_index("core")

    def both(d):
        give = part(d, 1 - core)
        got = swap(give)
        return part(d, core).astype(F32) + got.astype(F32)

    return both


def send(a, by):
    return shift(a.astype(BF), "x", by).astype(F32)


def sum_at_owner(part, base):
    both = halves_of(part)
    arrived = [send(both(d), d) for d in (2, 1, 3)]
    return base + both(0) + arrived[0] + arrived[1] + arrived[2]


def sum_by_neighbours(part, base):
    both = halves_of(part)
    half = base.shape[0] // 2
    across = both(2)
    above = send(across[:half], 1)
    below = send(across[half:], 3)
    up = both(1)
    up_lower = send(up[half:], 1)
    down = both(3)
    down_upper = send(down[:half], 3)
    up_upper = send(up[:half] + above, 1)
    down_lower = send(down[half:] + below, 3)
    own = base + both(0)
    return jnp.concatenate([own[:half] + up_upper + down_upper, own[half:] + up_lower + down_lower])


def earlier_blocks(state, fillers):
    z, y = lax.axis_index("z"), lax.axis_index("y")
    other = lax.ppermute(state, "z", [(i, i ^ 1) for i in range(lax.axis_size("z"))]).astype(F32)
    row = state.astype(F32) + other
    before = jnp.where(z % 2 == 1, other, 0.0)
    pair = row.astype(BF)
    found = [shift(pair, "z", d) for d in (4, 2, 6)]
    filled = fillers()
    *found, filled = lax.optimization_barrier((*found, filled))
    for d, s in zip((4, 2, 6), found):
        s = s.astype(F32)
        row = row + s
        before = before + jnp.where(z >= d, s, 0.0)
    row = row.astype(BF)
    for d in (2, 1, 3):
        before = before + jnp.where(y >= d, shift(row, "y", d).astype(F32), 0.0)
    return before.astype(BF), filled


def body(tokens, w_query, w_key, w_value, head_gain, w_out, norm_gain, w_gate, w_up, w_down):
    length = tokens.shape[0]
    width = norm_gain.shape[0]
    heads = w_query.shape[1] // HD
    ff = w_gate.shape[1]
    place = jnp.stack([lax.axis_index(a) for a in ("x", "core")]).astype(jnp.int32)
    packed = jnp.concatenate([w_gate, w_up, w_down.T], axis=1)
    weights = lax.all_gather(packed, SEQ, axis=0, tiled=True)
    mine, theirs = spread(tokens)
    rows, row = (length, W), (length, width)
    whole, keys, values, state = kernel_of(
        keys_kernel,
        [(row, BF), (rows, BF), (rows, BF), ((heads, HD, HD), BF)],
        place,
        *mine,
        *theirs,
        (w_key,),
        (w_value,),
        scratch=[
            pltpu.VMEM((width, W), BF),
            pltpu.VMEM((width, W), BF),
            pltpu.SemaphoreType.DMA((2,)),
        ],
        flops=4 * length * width * W,
    )

    def query_of():
        return kernel_of(
            query_kernel, [(rows, BF)], whole, w_query, flops=2 * length * width * W
        )[0]

    history, query = earlier_blocks(state, query_of)
    (inside,) = kernel_of(
        inside_kernel, [(rows, F32)], query, keys, values, flops=4 * length * length * W
    )
    (normed,) = kernel_of(
        mixed_kernel,
        [(rows, BF)],
        query,
        inside,
        history,
        head_gain.reshape(1, W),
        flops=2 * length * HD * W,
    )
    x = lax.axis_index("x")

    def attn(d, c):
        at = (2 * lax.rem(x + d, 4) + c) * W
        return dot(normed, lax.dynamic_slice_in_dim(w_out, at, W, 1)).astype(BF)

    resid = sum_at_owner(attn, tokens)
    mine, theirs = spread(resid.astype(BF))
    n = ff // W
    scaled, factor = kernel_of(
        prep_kernel,
        [(row, BF, pltpu.HBM), ((length, HD), F32, pltpu.HBM)],
        place,
        *mine,
        *theirs,
        norm_gain.reshape(1, width),
        scratch=[
            pltpu.VMEM(row, BF),
            pltpu.VMEM((length, HD), F32),
            pltpu.SemaphoreType.DMA((2,)),
        ],
        flops=4 * length * width,
    )
    hidden, downs = kernel_of(
        hidden_kernel,
        [((length, ff), BF), ((width, ff), BF)],
        (scaled,),
        (factor,),
        (weights,),
        scratch=[
            pltpu.VMEM(row, BF),
            pltpu.VMEM((length, HD), F32),
            pltpu.VMEM((n, width, W), BF),
            pltpu.VMEM((n, width, W), BF),
            pltpu.SemaphoreType.DMA((4, 4)),
        ],
        flops=4 * length * width * ff,
        grant=20,
    )

    def mlp(d, c):
        at = (2 * lax.rem(x + d, 4) + c) * W
        w = lax.dynamic_slice_in_dim(downs, at, W, 0)
        return dot(hidden, w, ((1,), (1,))).astype(BF)

    return sum_by_neighbours(mlp, resid).astype(BF)


def solution(mesh):
    finer = Mesh(mesh.devices.reshape(4, 8, 4, 2), SEQ + TP)
    return jax.shard_map(
        body,
        mesh=finer,
        in_specs=(
            P(SEQ, TP),
            P(None, TP),
            P(None, TP),
            P(None, TP),
            P(TP),
            P(TP, None),
            P(),
            P(SEQ, TP),
            P(SEQ, TP),
            P(TP, SEQ),
        ),
        out_specs=P(SEQ, TP),
        check_vma=False,
    )
```

```python
import functools

import jax
import jax.numpy as jnp
from jax import lax
from jax.experimental import pallas as pl
from jax.experimental.pallas import tpu as pltpu
from jax.sharding import Mesh
from jax.sharding import PartitionSpec as P


HD = 128
W = 256
SEQ = ("y", "z")
TP = ("x", "core")
BF = jnp.bfloat16
F32 = jnp.float32


def shift(a, axis, by):
    n = lax.axis_size(axis)
    return lax.ppermute(a, axis, [(i, (i + by) % n) for i in range(n)])


def swap(a):
    return shift(a, "core", 1)


def spread(t):
    mine, theirs = [t], []
    for d in (1, 2, 3):
        mine.append(shift(t, "x", d))
    for d in range(4):
        theirs.append(swap(mine[d]))
    return mine, theirs


def everyone(a, axis):
    n = lax.axis_size(axis)
    copies = jnp.broadcast_to(a[None], (n, *a.shape))
    got = lax.all_to_all(copies, axis, split_axis=0, concat_axis=0, tiled=True)
    return got.reshape(n * a.shape[0], *a.shape[1:])


def here(a):
    return pltpu.with_memory_space_constraint(a, pltpu.VMEM)


def kernel_of(body, out, *args, scratch=(), flops=0, grant=8):
    place = pl.BlockSpec(memory_space=pltpu.SMEM)
    vmem = pl.BlockSpec(memory_space=pltpu.VMEM)
    stays = pl.BlockSpec(memory_space=pltpu.HBM)
    specs, values = [], []
    for a in args:
        if isinstance(a, tuple):
            specs.append(stays)
            values.append(pltpu.with_memory_space_constraint(a[0], pltpu.HBM))
        elif a.dtype == jnp.int32:
            specs.append(place)
            values.append(a)
        else:
            specs.append(vmem)
            values.append(here(a))
    return pl.pallas_call(
        body,
        in_specs=specs,
        out_specs=[stays if space else vmem for _, _, *space in out],
        out_shape=[(space or [pltpu.VMEM])[0](shape, dtype) for shape, dtype, *space in out],
        scratch_shapes=list(scratch),
        compiler_params=pltpu.CompilerParams(vmem_limit_bytes=grant << 20),
        cost_estimate=pl.CostEstimate(flops=flops, bytes_accessed=8 << 20, transcendentals=0),
    )(*values)


def dot(a, b, dims=((1,), (0,))):
    return lax.dot_general(a, b, (dims, ((), ())), preferred_element_type=F32)


def pieces_of(place, mine, theirs):
    x, core = place[0], place[1]
    for d in range(4):
        chip = lax.rem(x + 4 - d, 4)
        yield pl.multiple_of((2 * chip + core) * W, W), mine[d]
        yield pl.multiple_of((2 * chip + 1 - core) * W, W), theirs[d]


def by_tiles(length, step):
    def run(i, _):
        step(pl.ds(pl.multiple_of(i * 256, 256), 256))
        return 0

    lax.fori_loop(0, length // 256, run, 0)


def keys_kernel(place, *refs):
    k_from, v_from, whole, keys, values, state, w_key, w_value, sems = refs[8:]
    load_k = pltpu.make_async_copy(k_from, w_key, sems.at[0])
    load_v = pltpu.make_async_copy(v_from, w_value, sems.at[1])
    load_k.start()
    load_v.start()

    @functools.partial(by_tiles, whole.shape[0])
    def _(rows):
        for at, piece in pieces_of(place, refs[:4], refs[4:8]):
            whole[rows, pl.ds(at, W)] = piece[rows, :]

    load_k.wait()
    load_v.wait()

    @functools.partial(by_tiles, whole.shape[0])
    def _(rows):
        keys[rows, :] = dot(whole[rows, :], w_key[...]).astype(BF)
        values[rows, :] = dot(whole[rows, :], w_value[...]).astype(BF)

    for h in range(2):
        cols = slice(h * HD, (h + 1) * HD)
        state[h] = dot(keys[:, cols], values[:, cols], ((0,), (0,))).astype(BF)


def query_kernel(whole, w_query, query):
    @functools.partial(by_tiles, whole.shape[0])
    def _(rows):
        query[rows, :] = dot(whole[rows, :], w_query[...]).astype(BF)


def inside_kernel(query, keys, values, inside):
    length = keys.shape[0]

    @functools.partial(by_tiles, length)
    def _(rows):
        i = lax.broadcasted_iota(jnp.int32, (256, length), 0) + rows.start
        j = lax.broadcasted_iota(jnp.int32, (256, length), 1)
        for h in range(2):
            cols = slice(h * HD, (h + 1) * HD)
            s = dot(query[rows, cols], keys[:, cols], ((1,), (1,)))
            s = jnp.where(i >= j, s, 0.0).astype(BF)
            inside[rows, cols] = dot(s, values[:, cols])


def mixed_kernel(query, inside, history, head_gain, normed):
    @functools.partial(by_tiles, query.shape[0])
    def _(rows):
        for h in range(2):
            cols = slice(h * HD, (h + 1) * HD)
            m = inside[rows, cols] + dot(query[rows, cols], history[h])
            scale = lax.rsqrt(jnp.mean(m * m, axis=-1, keepdims=True) + 1e-06)
            normed[rows, cols] = (m * scale * head_gain[:, cols]).astype(BF)


def prep_kernel(place, *refs):
    norm_gain, scaled_out, factor_out, scaled, factor, sems = refs[8:]
    length, width = scaled.shape

    @functools.partial(by_tiles, length)
    def _(rows):
        total = jnp.zeros((256, W), F32)
        for at, piece in pieces_of(place, refs[:4], refs[4:8]):
            v = piece[rows, :].astype(F32)
            total = total + v * v
            scaled[rows, pl.ds(at, W)] = (v * norm_gain[:, pl.ds(at, W)]).astype(BF)
        mean = jnp.sum(total, axis=-1, keepdims=True) / width
        factor[rows, :] = jnp.broadcast_to(lax.rsqrt(mean + 1e-05), (256, factor.shape[1]))

    copies = [
        pltpu.make_async_copy(scaled, scaled_out, sems.at[0]),
        pltpu.make_async_copy(factor, factor_out, sems.at[1]),
    ]
    for c in copies:
        c.start()
    for c in copies:
        c.wait()


def hidden_kernel(place, scaled_from, factor_from, weights, *refs):
    *late, hidden, downs, x, factor, gate, up, sems = refs
    length, _ = x.shape
    ff = hidden.shape[1]

    def tile(s):
        at = pl.multiple_of(s * W, W)
        g = pltpu.make_async_copy(weights.at[:, pl.ds(at, W)], gate.at[s], sems.at[0, s])
        u = pltpu.make_async_copy(weights.at[:, pl.ds(ff + at, W)], up.at[s], sems.at[1, s])
        return g, u

    def rows_of(r):
        rows = pl.ds(r * W, W)
        return pltpu.make_async_copy(scaled_from.at[rows, :], x.at[rows, :], sems.at[2, r])

    scales = pltpu.make_async_copy(factor_from, factor, sems.at[2, 3])
    end = ff // W - 1
    deep = late[0].shape[0]
    last = pltpu.make_async_copy(weights.at[:, 2 * ff - W : 3 * ff - W], downs, sems.at[3, 0])
    rows_of(0).start()
    for c in tile(0):
        c.start()
    scales.start()
    for r in range(1, length // W):
        rows_of(r).start()
    for s in range(1, ff // W):
        g, u = tile(s)
        g.start()
        if s < end:
            u.start()
    for d, piece in enumerate(late):
        at = pl.multiple_of(lax.rem(place[2] + 4 - d, 4) * deep, deep)
        pltpu.make_async_copy(piece, up.at[end, pl.ds(at, deep), :], sems.at[1, end]).start()
    last.start()

    scales.wait()
    for r in range(length // W):
        rows_of(r).wait()

    def step(s, _):
        for c in tile(s):
            c.wait()
        cols = pl.ds(pl.multiple_of(s * W, W), W)

        for r in range(length // W):
            rows = slice(r * W, (r + 1) * W)
            f = jnp.concatenate([factor[rows, :]] * (W // factor.shape[1]), axis=1)
            g = dot(x[rows, :], gate[s]) * f
            u = dot(x[rows, :], up[s]) * f
            hidden[rows, cols] = (g / (1.0 + jnp.exp(-g)) * u).astype(BF)
        return 0

    lax.fori_loop(0, ff // W, step, 0)
    last.wait()


def halves_of(part):
    core = lax.axis_index("core")

    def both(d):
        give = part(d, 1 - core)
        got = swap(give)
        return part(d, core).astype(F32) + got.astype(F32)

    return both


def send(a, by):
    return shift(a.astype(BF), "x", by).astype(F32)


def sum_at_owner(part, base):
    both = halves_of(part)
    arrived = [send(both(d), d) for d in (2, 1, 3)]
    return base + both(0) + arrived[0] + arrived[1] + arrived[2]


def sum_by_neighbours(part, base):
    both = halves_of(part)
    half = base.shape[0] // 2
    across = both(2)
    above = send(across[:half], 1)
    below = send(across[half:], 3)
    up = both(1)
    up_lower = send(up[half:], 1)
    down = both(3)
    down_upper = send(down[:half], 3)
    up_upper = send(up[:half] + above, 1)
    down_lower = send(down[half:] + below, 3)
    own = base + both(0)
    return jnp.concatenate([own[:half] + up_upper + down_upper, own[half:] + up_lower + down_lower])


def earlier_blocks(state, fillers):
    z, y = lax.axis_index("z"), lax.axis_index("y")
    other = lax.ppermute(state, "z", [(i, i ^ 1) for i in range(lax.axis_size("z"))])
    other = other.astype(F32)
    row = state.astype(F32) + other
    before = jnp.where(z % 2 == 1, other, 0.0)
    pair = row.astype(BF)
    found = [shift(pair, "z", d) for d in (4, 2, 6)]
    filled = fillers()
    *found, filled = lax.optimization_barrier((*found, filled))
    for d, s in zip((4, 2, 6), found):
        s = s.astype(F32)
        row = row + s
        before = before + jnp.where(z >= d, s, 0.0)
    row = row.astype(BF)
    for d in (2, 1, 3):
        before = before + jnp.where(y >= d, shift(row, "y", d).astype(F32), 0.0)
    return before.astype(BF), filled


def body(tokens, w_query, w_key, w_value, head_gain, w_out, norm_gain, w_gate, w_up, w_down):
    length = tokens.shape[0]
    width = norm_gain.shape[0]
    heads = w_query.shape[1] // HD
    ff = w_gate.shape[1]
    place = jnp.stack([lax.axis_index(a) for a in ("x", "core", "y")]).astype(jnp.int32)
    packed = jnp.concatenate([w_gate, w_up[:, : ff - W], w_down.T], axis=1)
    weights = lax.all_gather(packed, SEQ, axis=0, tiled=True)
    mine, theirs = spread(tokens)
    column = everyone(w_up[:, ff - W :], "z")
    late = [column]
    for d in (1, 2, 3):
        late.append(shift(column, "y", d))
    rows, row = (length, W), (length, width)
    whole, keys, values, state = kernel_of(
        keys_kernel,
        [(row, BF), (rows, BF), (rows, BF), ((heads, HD, HD), BF)],
        place,
        *mine,
        *theirs,
        (w_key,),
        (w_value,),
        scratch=[
            pltpu.VMEM((width, W), BF),
            pltpu.VMEM((width, W), BF),
            pltpu.SemaphoreType.DMA((2,)),
        ],
        flops=4 * length * width * W,
    )

    def query_of():
        return kernel_of(
            query_kernel, [(rows, BF)], whole, w_query, flops=2 * length * width * W
        )[0]

    history, query = earlier_blocks(state, query_of)
    (inside,) = kernel_of(
        inside_kernel, [(rows, F32)], query, keys, values, flops=4 * length * length * W
    )
    (normed,) = kernel_of(
        mixed_kernel,
        [(rows, BF)],
        query,
        inside,
        history,
        head_gain.reshape(1, W),
        flops=2 * length * HD * W,
    )
    x = lax.axis_index("x")

    def attn(d, c):
        at = (2 * lax.rem(x + d, 4) + c) * W
        return dot(normed, lax.dynamic_slice_in_dim(w_out, at, W, 1)).astype(BF)

    resid = sum_at_owner(attn, tokens)
    mine, theirs = spread(resid.astype(BF))
    n = ff // W
    scaled, factor = kernel_of(
        prep_kernel,
        [(row, BF, pltpu.HBM), ((length, HD), F32, pltpu.HBM)],
        place,
        *mine,
        *theirs,
        norm_gain.reshape(1, width),
        scratch=[
            pltpu.VMEM(row, BF),
            pltpu.VMEM((length, HD), F32),
            pltpu.SemaphoreType.DMA((2,)),
        ],
        flops=4 * length * width,
    )
    hidden, downs = kernel_of(
        hidden_kernel,
        [((length, ff), BF), ((width, ff), BF)],
        place,
        (scaled,),
        (factor,),
        (weights,),
        *[(p,) for p in late],
        scratch=[
            pltpu.VMEM(row, BF),
            pltpu.VMEM((length, HD), F32),
            pltpu.VMEM((n, width, W), BF),
            pltpu.VMEM((n, width, W), BF),
            pltpu.SemaphoreType.DMA((4, 4)),
        ],
        flops=4 * length * width * ff,
        grant=20,
    )

    def mlp(d, c):
        at = (2 * lax.rem(x + d, 4) + c) * W
        w = lax.dynamic_slice_in_dim(downs, at, W, 0)
        return dot(hidden, w, ((1,), (1,))).astype(BF)

    return sum_by_neighbours(mlp, resid).astype(BF)


def solution(mesh):
    finer = Mesh(mesh.devices.reshape(4, 8, 4, 2), SEQ + TP)
    return jax.shard_map(
        body,
        mesh=finer,
        in_specs=(
            P(SEQ, TP),
            P(None, TP),
            P(None, TP),
            P(None, TP),
            P(TP),
            P(TP, None),
            P(),
            P(SEQ, TP),
            P(SEQ, TP),
            P(TP, SEQ),
        ),
        out_specs=P(SEQ, TP),
        check_vma=False,
    )
```
